32 devices in a mesh: parts: 2 (over x), seq: 16 (over z, y, core).
Axes of the slice: x: 2, y: 2, z: 4, core: 2. Of those that a mesh axis runs over, the one named last changes fastest.
Arguments:
- tokens: bfloat16 [16384, 2560], P(('parts', 'seq')), parts along dimension 0, may hold values from -6 to 6
- lengths: int32 [32], P('parts'), parts along dimension 0, may hold values from 1 to 2048, 8192 in all
- gate_value_proj: bfloat16 [2560, 1280], replicated, may hold values from -0.125 to 0.125
- state_proj: bfloat16 [2560, 256], replicated, may hold values from -0.125 to 0.125
- step_proj: bfloat16 [2560, 10], replicated, may hold values from -0.125 to 0.125
- step_bias: float32 [10], replicated, may hold values from -3 to -1
- decay_log: float32 [10], replicated, may hold values from -8 to -1
- conv_weight: float32 [4, 896], replicated, may hold values from -3 to 3
- conv_bias: float32 [896], replicated, may hold values from -3 to 3
- skip_gain: float32 [10], replicated, may hold values from 0.5 to 2
- norm_gain: float32 [640], replicated, may hold values from 0.1 to 1.9
Outputs:
- normed: bfloat16 [16384, 640], P(('parts', 'seq')), parts along dimension 0
The draws below stay inside these ranges and needn't reach their ends.
There are 2 independent parts, one for each index of `parts`. The reference program is written for one: setup_inputs(seed, part) draws one part's arguments, and reference() takes and returns one part's arrays. A program takes and returns all parts, laid end to end along the dimension named above; an argument that names none is the same for every part. Nothing has to cross between parts.
Inputs may be any that keep to these rules, and one draw needn't show every extreme that they name: The 16 lengths sum to 8192; the longest is exactly 2048.
All inputs are finite; a program needn't handle non-finite values.
Results may differ from the reference program's by a relative error of at most 0.0055.
Values may be sent and summed in bfloat16 or wider, within the bound.
A program may use at most 128 MiB of HBM per device.

```python
import math
import jax
import jax.numpy as jnp
import numpy as np
from jax import lax

D = 2560
HEADS = 10
STATE = 128
SPAN = 256
INNER = 640
TOKENS = 8192
DOCS = 16


def block_levels(rng, shape, split, low, top_value):
    gain = 1.0
    for dim, parts in split:
        draws = jax.random.uniform(jax.random.fold_in(jax.random.fold_in(rng, 6), dim), (parts,), jnp.float32, low / len(split), top_value / len(split))
        gain = gain * jnp.repeat(jnp.exp(draws), shape[dim] // parts).reshape((-1,) + (1,) * (len(shape) - 1 - dim))
    return gain


def length_profile(amount, total, limit, slope):
    weights = [(1 << 20) // math.isqrt(grade ** slope) + 1 for grade in range(2, amount + 1)]
    surplus, counts = total - limit - (amount - 1), [1] * (amount - 1)
    while surplus > 0:
        movable = [i for i in range(amount - 1) if counts[i] < limit]
        whole, remaining = sum([weights[i] for i in movable]), surplus
        for i in movable:
            more = min(limit - counts[i], max(1, remaining * weights[i] // whole), surplus)
            counts[i] = counts[i] + more
            surplus = surplus - more
    return np.array([limit] + counts)


def ragged_sizes(rng, amount, total, reach, lean):
    if amount == 2:
        one = jax.random.randint(rng, (), max(1, total - reach), min(reach, total - 1) + 1)
        return jnp.stack([one, total - one])
    tallies = jnp.asarray(length_profile(amount, total, reach, lean), jnp.int32)
    twos = (amount - 1) // 2
    donor, receiver = tallies[1:1 + 2 * twos:2], tallies[2:2 + 2 * twos:2]
    room = jnp.minimum(donor - 1, reach - receiver)
    moved = jax.random.randint(jax.random.fold_in(rng, 1), (twos,), 0, 1 << 20) % (room + 1)
    tallies = tallies.at[1:1 + 2 * twos:2].set(donor - moved).at[2:2 + 2 * twos:2].set(receiver + moved)
    return tallies[jax.random.permutation(jax.random.fold_in(rng, 2), amount)]


def gaussian(stream_key, dims, scale, bound, pieces=(), kind=jnp.bfloat16):
    array = jax.random.normal(stream_key, dims, jnp.float32) * scale
    if len(pieces) > 0:
        array = block_levels(stream_key, dims, pieces, -0.22, 0.18) * array
    return jnp.clip(array, min=-bound, max=bound).astype(kind)


def setup_inputs(seed: int = 0, part: int = 0) -> dict:
    arg_keys = jax.random.split(jax.random.key(seed), 12)
    part_keys = jax.random.split(jax.random.fold_in(arg_keys[11], part), 12)
    tokens = gaussian(part_keys[0], (TOKENS, D), 1.0, 6.0, ((0, 16),))
    lengths = ragged_sizes(part_keys[1], DOCS, TOKENS, TOKENS // 4, 2).astype(jnp.int32)
    gate_value_proj = gaussian(arg_keys[2], (D, 2 * INNER), D ** -0.5, 0.125)
    state_proj = gaussian(arg_keys[3], (D, 2 * STATE), D ** -0.5, 0.125)
    step_proj = gaussian(arg_keys[4], (D, HEADS), D ** -0.5, 0.125)
    step_bias = jnp.clip(jax.random.uniform(arg_keys[5], (HEADS,), jnp.float32, -3.0, -1.0), -3.0, -1.0)
    decay_log = jnp.clip(jax.random.uniform(arg_keys[6], (HEADS,), jnp.float32, -8.0, -1.0), -8.0, -1.0)
    conv_weight = gaussian(arg_keys[7], (4, INNER + 2 * STATE), 0.5, 3.0, (), jnp.float32)
    conv_bias = gaussian(arg_keys[8], (INNER + 2 * STATE,), 0.5, 3.0, (), jnp.float32)
    skip_gain = jnp.clip(jax.random.uniform(arg_keys[9], (HEADS,), jnp.float32, 0.5, 2.0), 0.5, 2.0)
    norm_gain = jnp.clip(1.0 + 0.18 * jax.random.normal(arg_keys[10], (INNER,), jnp.float32), 0.1, 1.9)
    return {"tokens": tokens, "lengths": lengths, "gate_value_proj": gate_value_proj, "state_proj": state_proj, "step_proj": step_proj, "step_bias": step_bias, "decay_log": decay_log, "conv_weight": conv_weight, "conv_bias": conv_bias, "skip_gain": skip_gain, "norm_gain": norm_gain}


highest = lax.Precision.HIGHEST

def segment_of(lengths, positions):
    doc_ends = jnp.cumsum(lengths)
    doc_starts = doc_ends - lengths
    return lax.optimization_barrier(jnp.sum((doc_starts[None, :] <= positions[:, None]).astype(jnp.int32), axis=1)) - 1

def convolve(padded, pad_segment, conv_weight, conv_bias):
    row_count = padded.shape[0] - 3
    own_segment = pad_segment[3:]
    summed = conv_bias[None, :] + conv_weight[3][None, :] * padded[3:]
    for offset_tap in range(3):
        allowed = (pad_segment[offset_tap:offset_tap + row_count] == own_segment).astype(jnp.float32)
        summed = summed + allowed[:, None] * conv_weight[offset_tap][None, :] * padded[offset_tap:offset_tap + row_count]
    return jax.nn.silu(summed).astype(jnp.bfloat16)

def prepare(convolved, steps_raw, step_bias, decay_log, inner_width, head_count, state_width):
    row_count = convolved.shape[0]
    as_float = convolved.astype(jnp.float32)
    head_input = as_float[:, :inner_width].reshape(row_count, head_count, inner_width // head_count)
    in_map = as_float[:, inner_width:inner_width + state_width]
    out_map = as_float[:, inner_width + state_width:]
    step_size = jax.nn.softplus(steps_raw + step_bias[None, :])
    log_decay = -step_size * jnp.exp(decay_log)[None, :]
    return (head_input, in_map, out_map, log_decay, step_size)

def advance(carried, block):
    head_input, in_map, out_map, log_decay, step_size, segment, prev_segment = block
    length = segment.shape[0]
    cumulative = jnp.cumsum(log_decay, axis=0)
    order = jnp.arange(length, dtype=jnp.int32)
    allowed = (segment[:, None] == segment[None, :]) & (order[:, None] >= order[None, :])
    spread_log = jnp.minimum(cumulative[:, None, :] - cumulative[None, :, :], 0.0)
    weights = jnp.where(allowed[:, :, None], jnp.exp(spread_log), 0.0)
    scores = jnp.dot(out_map, in_map.T, precision=highest)
    mixing = weights * scores[:, :, None] * step_size[None, :, :]
    outputs = jnp.einsum('tsh,shp->thp', mixing, head_input, precision=highest)
    reached = (segment == prev_segment).astype(jnp.float32)
    entering = reached[:, None] * jnp.exp(cumulative)
    outputs = outputs + entering[:, :, None] * jnp.einsum('tn,hpn->thp', out_map, carried, precision=highest)
    final_segment = segment[length - 1]
    leaving = jnp.where((segment == final_segment)[:, None], jnp.exp(cumulative[length - 1][None, :] - cumulative), 0.0) * step_size
    carried = (reached[length - 1] * jnp.exp(cumulative[length - 1]))[:, None, None] * carried + jnp.einsum('sh,shp,sn->hpn', leaving, head_input, in_map, precision=highest)
    return (carried, outputs)

def finish(outputs, head_input, skip_gain, gate_raw, norm_gain):
    row_count = outputs.shape[0]
    outputs = outputs + skip_gain[None, :, None] * head_input
    gated = outputs.reshape(row_count, -1) * jax.nn.silu(gate_raw.astype(jnp.float32))
    normed = gated * lax.rsqrt(lax.optimization_barrier(jnp.mean(gated * gated, axis=1, keepdims=True)) + 1e-05) * norm_gain[None, :]
    return normed.astype(jnp.bfloat16)

def reference(tokens, lengths, gate_value_proj, state_proj, step_proj, step_bias, decay_log, conv_weight, conv_bias, skip_gain, norm_gain):
    row_count = tokens.shape[0]
    inner_width = gate_value_proj.shape[1] // 2
    state_width = state_proj.shape[1] // 2
    head_count = step_proj.shape[1]
    head_width = inner_width // head_count
    projected = jnp.dot(tokens, gate_value_proj, preferred_element_type=jnp.float32).astype(jnp.bfloat16)
    state_maps = jnp.dot(tokens, state_proj, preferred_element_type=jnp.float32).astype(jnp.bfloat16)
    steps_raw = jnp.dot(tokens, step_proj, preferred_element_type=jnp.float32)
    mixed_in = jnp.concatenate([projected[:, inner_width:], state_maps], axis=1)
    padded = jnp.concatenate([jnp.zeros((3, mixed_in.shape[1]), jnp.float32), mixed_in.astype(jnp.float32)], axis=0)
    positions = jnp.arange(row_count + 3, dtype=jnp.int32) - 3
    pad_segment = segment_of(lengths, positions)
    convolved = convolve(padded, pad_segment, conv_weight, conv_bias)
    head_input, in_map, out_map, log_decay, step_size = prepare(convolved, steps_raw, step_bias, decay_log, inner_width, head_count, state_width)
    segment = pad_segment[3:]
    blocks = row_count // SPAN
    prev_segments = pad_segment[2:2 + row_count:SPAN]
    block = (head_input.reshape(blocks, SPAN, head_count, head_width), in_map.reshape(blocks, SPAN, state_width), out_map.reshape(blocks, SPAN, state_width), log_decay.reshape(blocks, SPAN, head_count), step_size.reshape(blocks, SPAN, head_count), segment.reshape(blocks, SPAN), prev_segments)
    carried, outputs = lax.scan(advance, jnp.zeros((head_count, head_width, state_width), jnp.float32), block)
    outputs = outputs.reshape(row_count, head_count, head_width)
    return finish(outputs, head_input, skip_gain, projected[:, :inner_width], norm_gain)
```

```python
import functools

import jax
import jax.numpy as jnp
from jax import lax
from jax.experimental import pallas as pl
from jax.experimental.pallas import tpu as pltpu
from jax.sharding import PartitionSpec as P

CHUNK = 128
LANES = 128
HALO = 16
COLS = 256
MESH = pl.DeviceIdType.MESH
f32 = jnp.float32
bf16 = jnp.bfloat16


def split3(x):
    hi = x.astype(bf16)
    rest = x - hi.astype(f32)
    mid = rest.astype(bf16)
    return hi, mid, (rest - mid.astype(f32)).astype(bf16)


def expanded(x, spread):
    hi = x.astype(bf16)
    lo = (x - hi.astype(f32)).astype(bf16)
    return jnp.dot(jnp.concatenate([hi, lo], axis=1), spread, preferred_element_type=f32)


def half_silu(h):
    return h + h * jnp.tanh(h)


def kernel(
    n,
    span,
    tokens,
    lengths,
    gv_hbm,
    sp_hbm,
    stp_hbm,
    step_bias,
    decay_log,
    conv_weight,
    conv_bias,
    skip_gain,
    norm_gain,
    out,
    tok,
    gv,
    sp,
    stp,
    narrow,
    mixed,
    keep,
    conv,
    gate,
    ysum,
    enter,
    state32,
    state16,
    dec_mine,
    pair16,
    pair_dec,
    got_a,
    got_a_dec,
    got_b,
    got_b_dec,
    enter16,
    full16,
    load_sem,
    halo_sem,
    a_sem,
    b_send,
    b_recv,
    c_sem,
):
    rows = tokens.shape[0]
    inner = gate.shape[1]
    width = conv.shape[1]
    state = (width - inner) // 2
    half = state // 2
    heads = stp.shape[0]
    head = inner // heads
    docs = lengths.shape[0]
    chunks = rows // CHUNK
    me = lax.axis_index("seq")
    core = lax.rem(me, 2)
    mate = me + 1 - 2 * core
    first = me * rows

    blocks = list(range(0, 2 * inner, COLS))
    order = [b for b in blocks if b + COLS > inner] + [b for b in blocks if b + COLS <= inner]
    loads = {}

    def load(name, src, dst):
        loads[name] = pltpu.make_async_copy(src, dst, load_sem.at[len(loads)])
        loads[name].start()

    load("tok", tokens, tok.at[pl.ds(HALO, rows)])
    load("stp", stp_hbm, stp)
    load("sp", sp_hbm, sp)
    for b in order:
        load(b, gv_hbm.at[:, pl.ds(b, COLS)], gv.at[:, pl.ds(b, COLS)])

    offsets = [-1, 1] + [s * 2 * k for k in range(1, span + 1) for s in (-1, 1)]
    barrier = pltpu.get_barrier_semaphore()
    for o in offsets:
        @pl.when((me + o >= 0) & (me + o < n))
        def _(o=o):
            pl.semaphore_signal(barrier, inc=1, device_id={"seq": me + o}, device_id_type=MESH)
    peers = jnp.int32(0)
    for o in offsets:
        peers = peers + jnp.where((me + o >= 0) & (me + o < n), 1, 0)
    pl.semaphore_wait(barrier, peers)

    halo = pltpu.make_async_remote_copy(
        src_ref=tokens.at[pl.ds(rows - HALO, HALO)],
        dst_ref=tok.at[pl.ds(0, HALO)],
        send_sem=halo_sem.at[0],
        recv_sem=halo_sem.at[1],
        device_id={"seq": lax.rem(me + 1, n)},
        device_id_type=MESH,
    )

    @pl.when(me + 1 < n)
    def _():
        halo.start()

    @pl.when(me == 0)
    def _():
        tok[0:HALO, :] = jnp.zeros((HALO, tok.shape[1]), tok.dtype)

    starts = []
    total = jnp.int32(0)
    for j in range(docs):
        starts.append(total)
        total = total + lengths[j]
    pos = first + lax.broadcasted_iota(jnp.int32, (rows, LANES), 0)
    begin = jnp.zeros((rows, LANES), jnp.int32)
    for s in starts[1:]:
        begin = jnp.where(pos >= s, s, begin)

    def begin_of(p):
        b = jnp.int32(0)
        for s in starts[1:]:
            b = jnp.where(p >= s, s, b)
        return b

    for k in range(3):
        keep[k] = (pos - 3 + k >= begin).astype(f32)

    r = lax.broadcasted_iota(jnp.int32, (2 * LANES, inner), 0)
    c = lax.broadcasted_iota(jnp.int32, (2 * LANES, inner), 1)
    spread = (lax.rem(r, LANES) == c // head).astype(bf16)
    row_i = lax.broadcasted_iota(jnp.int32, (CHUNK, CHUNK), 0)
    col_i = lax.broadcasted_iota(jnp.int32, (CHUNK, CHUNK), 1)
    lower = (row_i >= col_i).astype(bf16)
    lower3 = jnp.concatenate([lower, lower, lower], axis=1)

    narrow[...] = jnp.zeros_like(narrow)
    loads["tok"].wait()
    loads["stp"].wait()
    own = tok.at[pl.ds(HALO, rows)]
    raw = lax.dot_general(
        own[...], stp[...], (((1,), (1,)), ((), ())), preferred_element_type=f32
    )
    narrow[0:rows, 0:heads] = raw
    narrow[rows : rows + 1, 0:heads] = step_bias[...]
    narrow[rows + 8 : rows + 9, 0:heads] = decay_log[...]
    narrow[rows + 16 : rows + 17, 0:heads] = skip_gain[...]
    live = lax.broadcasted_iota(jnp.int32, (rows, LANES), 1) < heads
    shifted = narrow[0:rows, :] + narrow[rows : rows + 1, :]
    step = jnp.maximum(shifted, 0.0) + jnp.log1p(jnp.exp(-jnp.abs(shifted)))
    step = jnp.where(live, step, 0.0)
    log_decay = -step * jnp.exp(narrow[rows + 8 : rows + 9, :])
    skip_row = expanded(narrow[rows + 16 : rows + 24, :], spread)[0:1]
    hi, mid, lo = split3(log_decay)
    cums, cums_t, steps_t, leaving, entering = [], [], [], [], []
    for ch in range(chunks):
        at = slice(ch * CHUNK, (ch + 1) * CHUNK)
        cum = jnp.dot(
            lower3,
            jnp.concatenate([hi[at], mid[at], lo[at]], axis=0),
            preferred_element_type=f32,
        )
        cums.append(cum)
        cums_t.append(cum.T)
        steps_t.append(step[at].T)
        chunk_first = first + ch * CHUNK
        last_begin = begin_of(chunk_first + CHUNK - 1)
        leaving.append(
            jnp.where(
                pos[at] >= last_begin, jnp.exp(cum[CHUNK - 1 : CHUNK] - cum), 0.0
            )
            * step[at]
        )
        entering.append(jnp.where(begin[at] < chunk_first, jnp.exp(cum), 0.0))
    leave_wide = []
    for ch in range(chunks):
        at = slice(ch * CHUNK, (ch + 1) * CHUNK)
        leave_wide.append(expanded(leaving[ch], spread))
        enter[at, :] = expanded(entering[ch], spread)

    bias_row = 0.5 * conv_bias[...].reshape(1, width)
    gain_row = norm_gain[...].reshape(1, inner)

    def convolve(lo_col, count):
        cols = slice(lo_col, lo_col + count)
        w = 0.5 * conv_weight[:, cols]
        h = bias_row[:, cols] + w[3:4] * mixed[HALO : HALO + rows, cols]
        for k in range(3):
            kept = keep[k]
            if count != LANES:
                kept = jnp.concatenate([kept] * (count // LANES), axis=1)
            h = h + w[k : k + 1] * (
                kept * mixed[HALO - 3 + k : HALO - 3 + k + rows, cols]
            )
        conv[:, cols] = half_silu(h).astype(bf16)

    @pl.when(me > 0)
    def _():
        halo.wait_recv()

    loads["sp"].wait()
    both = jnp.dot(tok[...], sp[...], preferred_element_type=f32)
    mixed[:, inner:width] = both.astype(bf16).astype(f32)
    pending = [(inner, width - inner)]
    for b in order:
        if b + COLS <= inner:
            continue
        loads[b].wait()
        got = jnp.dot(tok[...], gv[:, b : b + COLS], preferred_element_type=f32)
        got = got.astype(bf16).astype(f32)
        gates = max(0, inner - b)
        if gates:
            gate[:, b:inner] = half_silu(0.5 * got[HALO:, :gates])
        mixed[:, b + gates - inner : b + COLS - inner] = got[:, gates:]
        for p in pending:
            convolve(*p)
        pending = [(b + gates - inner, COLS - gates)]
    for p in pending:
        convolve(*p)

    locals_ = []
    for ch in range(chunks):
        at = slice(ch * CHUNK, (ch + 1) * CHUNK)
        weighted = (conv[at, 0:inner].astype(f32) * leave_wide[ch]).astype(bf16)
        locals_.append(
            lax.dot_general(
                conv[at, inner : inner + state],
                weighted,
                (((0,), (0,)), ((), ())),
                preferred_element_type=f32,
            )
        )
    decs = [enter[(ch + 1) * CHUNK - 1 : (ch + 1) * CHUNK, :] for ch in range(chunks)]
    device_state = locals_[0]
    device_dec = decs[0]
    for ch in range(1, chunks):
        device_state = decs[ch] * device_state + locals_[ch]
        device_dec = decs[ch] * device_dec
    for ch in range(chunks):
        state32[ch] = locals_[ch]
    state32[chunks] = device_state
    state16[...] = device_state.astype(bf16)

    def put_row(ref, row):
        for j in range(inner // LANES):
            ref[j : j + 1, :] = row[:, j * LANES : (j + 1) * LANES]

    def get_row(block):
        return jnp.concatenate([block[j : j + 1] for j in range(inner // LANES)], axis=1)

    put_row(dec_mine, device_dec)
    mine_at = pl.multiple_of(core * half, half)
    mate_at = pl.multiple_of((1 - core) * half, half)

    def remote(src, dst, send, recv, target):
        return pltpu.make_async_remote_copy(
            src_ref=src,
            dst_ref=dst,
            send_sem=send,
            recv_sem=recv,
            device_id={"seq": target},
            device_id_type=MESH,
        )

    a_copy = remote(state16.at[pl.ds(mate_at, half)], got_a, a_sem.at[0], a_sem.at[1], mate)
    a_dec = remote(dec_mine, got_a_dec, a_sem.at[2], a_sem.at[3], mate)
    a_copy.start()
    a_dec.start()

    def inside(ch):
        at = slice(ch * CHUNK, (ch + 1) * CHUNK)
        in_map = conv[at, inner : inner + state]
        out_map = conv[at, inner + state : width]
        scores = lax.dot_general(
            out_map, in_map, (((1,), (1,)), ((), ())), preferred_element_type=f32
        )
        allowed = (row_i >= col_i) & (first + ch * CHUNK + col_i >= begin[at])
        lane = lax.broadcasted_iota(jnp.int32, (CHUNK, LANES), 1)
        per = LANES // head
        for tile in range(inner // LANES):
            x = conv[at, tile * LANES : (tile + 1) * LANES]
            mixes, values = [], []
            for i in range(per):
                h = tile * per + i
                diff = jnp.minimum(cums[ch][:, h : h + 1] - cums_t[ch][h : h + 1, :], 0.0)
                weight = jnp.where(allowed, jnp.exp(diff), 0.0)
                mixes.append((weight * scores * steps_t[ch][h : h + 1, :]).astype(bf16))
                values.append(jnp.where(lane // head == i, x, jnp.zeros_like(x)))
            y = jnp.dot(
                jnp.concatenate(mixes, axis=1),
                jnp.concatenate(values, axis=0),
                preferred_element_type=f32,
            )
            cols = slice(tile * LANES, (tile + 1) * LANES)
            ysum[at, cols] = y + skip_row[:, cols] * x.astype(f32)

    inside(0)

    a_copy.wait()
    a_dec.wait()
    theirs = got_a[...].astype(f32)
    theirs_dec = get_row(got_a_dec[...])
    mine = state32[chunks, pl.ds(mine_at, half), :]
    even = core == 0
    early = jnp.where(even, mine, theirs)
    early_dec = jnp.where(even, device_dec, theirs_dec)
    late = jnp.where(even, theirs, mine)
    late_dec = jnp.where(even, theirs_dec, device_dec)
    pair16[...] = (late + late_dec * early).astype(bf16)
    put_row(pair_dec, late_dec * early_dec)

    b_copies = []
    for k in range(1, span + 1):
        target = lax.rem(me + 2 * k, n)
        b_copies.append(
            (
                remote(pair16, got_b.at[k - 1], b_send.at[2 * k - 2], b_recv.at[2 * k - 2], target),
                remote(
                    pair_dec, got_b_dec.at[k - 1], b_send.at[2 * k - 1], b_recv.at[2 * k - 1], target
                ),
            )
        )
    for k in range(1, span + 1):
        @pl.when(me + 2 * k < n)
        def _(k=k):
            for cp in b_copies[k - 1]:
                cp.start()

        @pl.when(me - 2 * k < 0)
        def _(k=k):
            got_b[k - 1] = jnp.zeros(got_b.shape[1:], bf16)
            got_b_dec[k - 1] = jnp.zeros(got_b_dec.shape[1:], f32)

    for b in order:
        if b + COLS > inner:
            continue
        loads[b].wait()
        got = jnp.dot(own[...], gv[:, b : b + COLS], preferred_element_type=f32)
        gate[:, b : b + COLS] = half_silu(0.5 * got.astype(bf16).astype(f32))
    for ch in range(1, chunks):
        inside(ch)

    for k in range(1, span + 1):
        @pl.when(me - 2 * k >= 0)
        def _(k=k):
            for cp in b_copies[k - 1]:
                cp.wait_recv()
    chip = jnp.zeros((half, inner), f32)
    for k in range(span, 0, -1):
        chip = got_b[k - 1].astype(f32) + get_row(got_b_dec[k - 1]) * chip
    second = early + early_dec * chip
    full16[pl.ds(mine_at, half), :] = jnp.where(even, chip, second).astype(bf16)
    enter16[...] = jnp.where(even, second, chip).astype(bf16)
    c_copy = remote(enter16, full16.at[pl.ds(mine_at, half)], c_sem.at[0], c_sem.at[1], mate)
    c_copy.start()
    c_copy.wait()

    carried = full16[...].astype(f32)
    for ch in range(chunks):
        at = slice(ch * CHUNK, (ch + 1) * CHUNK)
        off = jnp.dot(
            conv[at, inner + state : width], carried.astype(bf16), preferred_element_type=f32
        )
        gated = (ysum[at, :] + enter[at, :] * off) * gate[at, :]
        square = jnp.sum(gated * gated, axis=1, keepdims=True) * (1.0 / inner)
        out[at, :] = (gated * lax.rsqrt(square + 1e-05) * gain_row).astype(bf16)
        if ch + 1 < chunks:
            carried = decs[ch] * carried + state32[ch]

    @pl.when(me + 1 < n)
    def _():
        halo.wait_send()

    for k in range(1, span + 1):
        @pl.when(me + 2 * k < n)
        def _(k=k):
            for cp in b_copies[k - 1]:
                cp.wait_send()


def shards(
    tokens,
    lengths,
    gate_value_proj,
    state_proj,
    step_proj,
    step_bias,
    decay_log,
    conv_weight,
    conv_bias,
    skip_gain,
    norm_gain,
):
    rows, depth = tokens.shape
    inner = gate_value_proj.shape[1] // 2
    state = state_proj.shape[1] // 2
    heads = step_proj.shape[1]
    width = inner + 2 * state
    n = lax.axis_size("seq")
    span = max(1, n // 8)
    hbm = pl.BlockSpec(memory_space=pl.ANY)
    vmem = pl.BlockSpec(memory_space=pltpu.VMEM)
    half = state // 2
    small = (8, LANES)
    chunks = rows // CHUNK
    dma = pltpu.SemaphoreType.DMA
    blocks = 2 * inner // COLS
    return pl.pallas_call(
        functools.partial(kernel, n, span),
        out_shape=jax.ShapeDtypeStruct((rows, inner), bf16),
        in_specs=[hbm, pl.BlockSpec(memory_space=pltpu.SMEM), hbm, hbm, hbm] + [vmem] * 6,
        out_specs=vmem,
        scratch_shapes=[
            pltpu.VMEM((rows + HALO, depth), bf16),
            pltpu.VMEM((depth, 2 * inner), bf16),
            pltpu.VMEM((depth, 2 * state), bf16),
            pltpu.VMEM((heads, depth), bf16),
            pltpu.VMEM((rows + 24, LANES), f32),
            pltpu.VMEM((rows + HALO, width), f32),
            pltpu.VMEM((3, rows, LANES), f32),
            pltpu.VMEM((rows, width), bf16),
            pltpu.VMEM((rows, inner), f32),
            pltpu.VMEM((rows, inner), f32),
            pltpu.VMEM((rows, inner), f32),
            pltpu.VMEM((chunks + 1, state, inner), f32),
            pltpu.VMEM((state, inner), bf16),
            pltpu.VMEM(small, f32),
            pltpu.VMEM((half, inner), bf16),
            pltpu.VMEM(small, f32),
            pltpu.VMEM((half, inner), bf16),
            pltpu.VMEM(small, f32),
            pltpu.VMEM((span, half, inner), bf16),
            pltpu.VMEM((span,) + small, f32),
            pltpu.VMEM((half, inner), bf16),
            pltpu.VMEM((state, inner), bf16),
            dma((3 + blocks,)),
            dma((2,)),
            dma((4,)),
            dma((2 * span,)),
            dma((2 * span,)),
            dma((2,)),
        ],
        compiler_params=pltpu.CompilerParams(
            collective_id=0, has_side_effects=True, vmem_limit_bytes=60 * 1024 * 1024
        ),
        name="layer",
    )(
        tokens,
        lengths,
        gate_value_proj,
        state_proj,
        step_proj.T,
        step_bias[None],
        decay_log[None],
        conv_weight,
        conv_bias,
        skip_gain[None],
        norm_gain,
    )


def solution(mesh):
    return jax.shard_map(
        shards,
        mesh=mesh,
        in_specs=(P(("parts", "seq"), None), P("parts")) + (P(),) * 9,
        out_specs=P(("parts", "seq"), None),
        check_vma=False,
    )
```

```python
import functools

import jax
import jax.numpy as jnp
from jax import lax
from jax.experimental import pallas as pl
from jax.experimental.pallas import tpu as pltpu
from jax.sharding import PartitionSpec as P

CHUNK = 128
LANES = 128
HALO = 16
COLS = 256
MESH = pl.DeviceIdType.MESH
f32 = jnp.float32
bf16 = jnp.bfloat16


def split3(x):
    hi = x.astype(bf16)
    rest = x - hi.astype(f32)
    mid = rest.astype(bf16)
    return hi, mid, (rest - mid.astype(f32)).astype(bf16)


def expanded(x, spread):
    hi = x.astype(bf16)
    lo = (x - hi.astype(f32)).astype(bf16)
    return jnp.dot(jnp.concatenate([hi, lo], axis=1), spread, preferred_element_type=f32)


def half_silu(h):
    return h + h * jnp.tanh(h)


def kernel(
    n,
    span,
    tokens,
    lengths_hbm,
    gv_hbm,
    sp_hbm,
    stp_hbm,
    step_bias_hbm,
    decay_log_hbm,
    conv_weight_hbm,
    conv_bias_hbm,
    skip_gain_hbm,
    norm_gain_hbm,
    out,
    lengths,
    step_bias,
    decay_log,
    conv_weight,
    conv_bias,
    skip_gain,
    norm_gain,
    leave,
    tok,
    gv,
    sp,
    stp,
    narrow,
    mixed,
    keep,
    conv,
    gate,
    ysum,
    enter,
    state32,
    state16,
    dec_mine,
    pair16,
    pair_dec,
    got_a,
    got_a_dec,
    got_b,
    got_b_dec,
    enter16,
    full16,
    load_sem,
    halo_sem,
    a_sem,
    b_send,
    b_recv,
    c_sem,
):
    rows = tokens.shape[0]
    inner = gate.shape[1]
    width = conv.shape[1]
    state = (width - inner) // 2
    half = state // 2
    heads = stp.shape[0]
    head = inner // heads
    docs = lengths.shape[0]
    chunks = rows // CHUNK
    me = lax.axis_index("seq")
    core = lax.rem(me, 2)
    mate = me + 1 - 2 * core
    first = me * rows

    blocks = list(range(0, 2 * inner, COLS))
    order = [b for b in blocks if b >= inner]
    order += [b for b in blocks if b < inner < b + COLS]
    order += [b for b in blocks if b + COLS <= inner]
    loads = {}

    def load(name, src, dst):
        loads[name] = pltpu.make_async_copy(src, dst, load_sem.at[len(loads)])
        loads[name].start()

    load("lengths", lengths_hbm, lengths)
    load("stp", stp_hbm, stp)
    load("tok", tokens, tok.at[pl.ds(HALO, rows)])
    smalls = [
        (step_bias_hbm, step_bias),
        (decay_log_hbm, decay_log),
        (skip_gain_hbm, skip_gain),
        (conv_weight_hbm, conv_weight),
    ]
    for src, dst in ((conv_bias_hbm, conv_bias), (norm_gain_hbm, norm_gain)):
        for i in range(0, src.shape[0], LANES):
            smalls.append((src.at[pl.ds(i, LANES)], dst.at[pl.ds(i, LANES)]))
    for i, (src, dst) in enumerate(smalls):
        load(("small", i), src, dst)
    load("sp", sp_hbm, sp)
    for b in order:
        load(b, gv_hbm.at[:, pl.ds(b, COLS)], gv.at[:, pl.ds(b, COLS)])

    offsets = [-1, 1] + [s * 2 * k for k in range(1, span + 1) for s in (-1, 1)]
    barrier = pltpu.get_barrier_semaphore()
    for o in offsets:
        @pl.when((me + o >= 0) & (me + o < n))
        def _(o=o):
            pl.semaphore_signal(barrier, inc=1, device_id={"seq": me + o}, device_id_type=MESH)
    peers = jnp.int32(0)
    for o in offsets:
        peers = peers + jnp.where((me + o >= 0) & (me + o < n), 1, 0)
    pl.semaphore_wait(barrier, peers)

    halo = pltpu.make_async_remote_copy(
        src_ref=tokens.at[pl.ds(rows - HALO, HALO)],
        dst_ref=tok.at[pl.ds(0, HALO)],
        send_sem=halo_sem.at[0],
        recv_sem=halo_sem.at[1],
        device_id={"seq": lax.rem(me + 1, n)},
        device_id_type=MESH,
    )

    @pl.when(me + 1 < n)
    def _():
        halo.start()

    @pl.when(me == 0)
    def _():
        tok[0:HALO, :] = jnp.zeros((HALO, tok.shape[1]), tok.dtype)

    loads["lengths"].wait()
    starts = []
    total = jnp.int32(0)
    for j in range(docs):
        starts.append(total)
        total = total + lengths[j]
    pos = first + lax.broadcasted_iota(jnp.int32, (rows, LANES), 0)
    begin = jnp.zeros((rows, LANES), jnp.int32)
    for s in starts[1:]:
        begin = jnp.where(pos >= s, s, begin)

    def begin_of(p):
        b = jnp.int32(0)
        for s in starts[1:]:
            b = jnp.where(p >= s, s, b)
        return b

    for k in range(3):
        keep[k] = (pos - 3 + k >= begin).astype(f32)

    r = lax.broadcasted_iota(jnp.int32, (2 * LANES, inner), 0)
    c = lax.broadcasted_iota(jnp.int32, (2 * LANES, inner), 1)
    spread = (lax.rem(r, LANES) == c // head).astype(bf16)
    row_i = lax.broadcasted_iota(jnp.int32, (CHUNK, CHUNK), 0)
    col_i = lax.broadcasted_iota(jnp.int32, (CHUNK, CHUNK), 1)
    lower = (row_i >= col_i).astype(bf16)
    lower3 = jnp.concatenate([lower, lower, lower], axis=1)

    narrow[...] = jnp.zeros_like(narrow)
    for i in range(len(smalls)):
        loads["small", i].wait()
    loads["stp"].wait()
    loads["tok"].wait()
    own = tok.at[pl.ds(HALO, rows)]
    raw = lax.dot_general(
        own[...], stp[...], (((1,), (1,)), ((), ())), preferred_element_type=f32
    )
    narrow[0:rows, 0:heads] = raw
    narrow[rows : rows + 1, 0:heads] = step_bias[...]
    narrow[rows + 8 : rows + 9, 0:heads] = decay_log[...]
    narrow[rows + 16 : rows + 17, 0:heads] = skip_gain[...]
    @pl.when(me > 0)
    def _():
        halo.wait_recv()

    loads["sp"].wait()
    both = jnp.dot(tok[...], sp[...], preferred_element_type=f32)
    mixed[:, inner:width] = both.astype(bf16).astype(f32)

    live = lax.broadcasted_iota(jnp.int32, (CHUNK, LANES), 1) < heads
    rate = jnp.exp(narrow[rows + 8 : rows + 9, :])
    skip_row = expanded(narrow[rows + 16 : rows + 24, :], spread)[0:1]
    cums, cums_t, steps_t = [], [], []
    for ch in range(chunks):
        at = slice(ch * CHUNK, (ch + 1) * CHUNK)
        shifted = narrow[at, :] + narrow[rows : rows + 1, :]
        step = jnp.maximum(shifted, 0.0) + jnp.log1p(jnp.exp(-jnp.abs(shifted)))
        step = jnp.where(live, step, 0.0)
        cum = jnp.dot(
            lower3, jnp.concatenate(split3(-step * rate), axis=0), preferred_element_type=f32
        )
        cums.append(cum)
        cums_t.append(cum.T)
        steps_t.append(step.T)
        chunk_first = first + ch * CHUNK
        last_begin = begin_of(chunk_first + CHUNK - 1)
        here = first + ch * CHUNK + row_i
        leave[at, :] = (
            jnp.where(here >= last_begin, jnp.exp(cum[CHUNK - 1 : CHUNK] - cum), 0.0) * step
        )
        reach = jnp.where(begin[at] < chunk_first, jnp.exp(cum), 0.0)
        enter[at, 0:LANES] = reach
        narrow[rows + 24 + ch : rows + 25 + ch, :] = reach[CHUNK - 1 : CHUNK]
    wide_decs = expanded(narrow[rows + 24 : rows + 24 + 8 * ((chunks + 7) // 8), :], spread)
    decs = [wide_decs[ch : ch + 1] for ch in range(chunks)]

    bias_row = 0.5 * conv_bias[0:width].reshape(1, width)
    gain_row = norm_gain[0:inner].reshape(1, inner)

    piece = 64

    def convolve(lo_col, count):
        for col in range(lo_col, lo_col + count, LANES):
            cols = slice(col, col + LANES)
            w = 0.5 * conv_weight[:, cols]
            bias = bias_row[:, cols]
            for at in range(0, rows, piece):
                h = bias + w[3:4] * mixed[HALO + at : HALO + at + piece, cols]
                for k in range(3):
                    low = HALO - 3 + k + at
                    h = h + w[k : k + 1] * (
                        keep[k, at : at + piece, :] * mixed[low : low + piece, cols]
                    )
                conv[at : at + piece, cols] = half_silu(h).astype(bf16)

    def states(lo_col, count):
        cols = slice(lo_col, lo_col + count)
        total = None
        for ch in range(chunks):
            at = slice(ch * CHUNK, (ch + 1) * CHUNK)
            weighted = conv[at, cols].astype(f32) * expanded(leave[at, :], spread[:, cols])
            own_state = lax.dot_general(
                conv[at, inner : inner + state],
                weighted.astype(bf16),
                (((0,), (0,)), ((), ())),
                preferred_element_type=f32,
            )
            state32[ch, :, cols] = own_state
            total = own_state if ch == 0 else decs[ch][:, cols] * total + own_state
        state32[chunks, :, cols] = total
        state16[:, cols] = total.astype(bf16)

    pending = [(inner, width - inner)]
    for b in order:
        if b + COLS <= inner:
            continue
        loads[b].wait()
        got = jnp.dot(tok[...], gv[:, b : b + COLS], preferred_element_type=f32)
        gates = max(0, inner - b)
        if gates:
            gate[:, b:inner] = 0.5 * got[HALO:, :gates].astype(bf16).astype(f32)
        mixed[:, b + gates - inner : b + COLS - inner] = (
            got[:, gates:].astype(bf16).astype(f32)
        )
        for p in pending:
            convolve(*p)
            if p[0] < inner:
                states(*p)
        pending = [(b + gates - inner, COLS - gates)]
    for p in pending:
        convolve(*p)
        states(*p)
    device_dec = decs[0]
    for ch in range(1, chunks):
        device_dec = decs[ch] * device_dec

    def put_row(ref, row):
        for j in range(inner // LANES):
            ref[j : j + 1, :] = row[:, j * LANES : (j + 1) * LANES]

    def get_row(block):
        return jnp.concatenate([block[j : j + 1] for j in range(inner // LANES)], axis=1)

    put_row(dec_mine, device_dec)
    mine_at = pl.multiple_of(core * half, half)
    mate_at = pl.multiple_of((1 - core) * half, half)

    def remote(src, dst, send, recv, target):
        return pltpu.make_async_remote_copy(
            src_ref=src,
            dst_ref=dst,
            send_sem=send,
            recv_sem=recv,
            device_id={"seq": target},
            device_id_type=MESH,
        )

    a_copy = remote(state16.at[pl.ds(mate_at, half)], got_a, a_sem.at[0], a_sem.at[1], mate)
    a_dec = remote(dec_mine, got_a_dec, a_sem.at[2], a_sem.at[3], mate)
    a_copy.start()
    a_dec.start()

    def inside(ch):
        at = slice(ch * CHUNK, (ch + 1) * CHUNK)
        in_map = conv[at, inner : inner + state]
        out_map = conv[at, inner + state : width]
        scores = lax.dot_general(
            out_map, in_map, (((1,), (1,)), ((), ())), preferred_element_type=f32
        )
        allowed = (row_i >= col_i) & (first + ch * CHUNK + col_i >= begin[at])
        lane = lax.broadcasted_iota(jnp.int32, (CHUNK, LANES), 1)
        per = LANES // head
        for tile in range(inner // LANES):
            x = conv[at, tile * LANES : (tile + 1) * LANES]
            mixes, values = [], []
            for i in range(per):
                h = tile * per + i
                diff = jnp.minimum(cums[ch][:, h : h + 1] - cums_t[ch][h : h + 1, :], 0.0)
                weight = jnp.where(allowed, jnp.exp(diff), 0.0)
                mixes.append((weight * scores * steps_t[ch][h : h + 1, :]).astype(bf16))
                values.append(jnp.where(lane // head == i, x, jnp.zeros_like(x)))
            y = jnp.dot(
                jnp.concatenate(mixes, axis=1),
                jnp.concatenate(values, axis=0),
                preferred_element_type=f32,
            )
            cols = slice(tile * LANES, (tile + 1) * LANES)
            ysum[at, cols] = y + skip_row[:, cols] * x.astype(f32)

    def widen(ch):
        at = slice(ch * CHUNK, (ch + 1) * CHUNK)
        enter[at, :] = expanded(enter[at, 0:LANES], spread)

    inside(0)

    a_copy.wait()
    a_dec.wait()
    theirs = got_a[...].astype(f32)
    theirs_dec = get_row(got_a_dec[...])
    mine = state32[chunks, pl.ds(mine_at, half), :]
    even = core == 0
    early = jnp.where(even, mine, theirs)
    early_dec = jnp.where(even, device_dec, theirs_dec)
    late = jnp.where(even, theirs, mine)
    late_dec = jnp.where(even, theirs_dec, device_dec)
    pair16[...] = (late + late_dec * early).astype(bf16)
    put_row(pair_dec, late_dec * early_dec)

    b_copies = []
    for k in range(1, span + 1):
        target = lax.rem(me + 2 * k, n)
        b_copies.append(
            (
                remote(pair16, got_b.at[k - 1], b_send.at[2 * k - 2], b_recv.at[2 * k - 2], target),
                remote(
                    pair_dec, got_b_dec.at[k - 1], b_send.at[2 * k - 1], b_recv.at[2 * k - 1], target
                ),
            )
        )
    for k in range(1, span + 1):
        @pl.when(me + 2 * k < n)
        def _(k=k):
            for cp in b_copies[k - 1]:
                cp.start()

        @pl.when(me - 2 * k < 0)
        def _(k=k):
            got_b[k - 1] = jnp.zeros(got_b.shape[1:], bf16)
            got_b_dec[k - 1] = jnp.zeros(got_b_dec.shape[1:], f32)

    for b in order:
        if b + COLS > inner:
            continue
        loads[b].wait()
        got = jnp.dot(own[...], gv[:, b : b + COLS], preferred_element_type=f32)
        gate[:, b : b + COLS] = 0.5 * got.astype(bf16).astype(f32)
    for ch in range(1, chunks):
        inside(ch)
    for ch in range(chunks):
        at = slice(ch * CHUNK, (ch + 1) * CHUNK)
        widen(ch)
        gate[at, :] = half_silu(gate[at, :])

    for k in range(1, span + 1):
        @pl.when(me - 2 * k >= 0)
        def _(k=k):
            for cp in b_copies[k - 1]:
                cp.wait_recv()
    chip = jnp.zeros((half, inner), f32)
    for k in range(span, 0, -1):
        chip = got_b[k - 1].astype(f32) + get_row(got_b_dec[k - 1]) * chip
    second = early + early_dec * chip
    full16[pl.ds(mine_at, half), :] = jnp.where(even, chip, second).astype(bf16)
    enter16[...] = jnp.where(even, second, chip).astype(bf16)
    c_copy = remote(enter16, full16.at[pl.ds(mine_at, half)], c_sem.at[0], c_sem.at[1], mate)
    c_copy.start()
    c_copy.wait()

    carried = full16[...].astype(f32)
    for ch in range(chunks):
        at = slice(ch * CHUNK, (ch + 1) * CHUNK)
        off = jnp.dot(
            conv[at, inner + state : width], carried.astype(bf16), preferred_element_type=f32
        )
        gated = (ysum[at, :] + enter[at, :] * off) * gate[at, :]
        square = jnp.sum(gated * gated, axis=1, keepdims=True) * (1.0 / inner)
        out[at, :] = (gated * lax.rsqrt(square + 1e-05) * gain_row).astype(bf16)
        if ch + 1 < chunks:
            carried = decs[ch] * carried + state32[ch]

    @pl.when(me + 1 < n)
    def _():
        halo.wait_send()

    for k in range(1, span + 1):
        @pl.when(me + 2 * k < n)
        def _(k=k):
            for cp in b_copies[k - 1]:
                cp.wait_send()


def shards(
    tokens,
    lengths,
    gate_value_proj,
    state_proj,
    step_proj,
    step_bias,
    decay_log,
    conv_weight,
    conv_bias,
    skip_gain,
    norm_gain,
):
    rows, depth = tokens.shape
    inner = gate_value_proj.shape[1] // 2
    state = state_proj.shape[1] // 2
    heads = step_proj.shape[1]
    width = inner + 2 * state
    n = lax.axis_size("seq")
    span = max(1, n // 8)
    hbm = pl.BlockSpec(memory_space=pl.ANY)
    vmem = pl.BlockSpec(memory_space=pltpu.VMEM)
    half = state // 2
    small = (8, LANES)
    chunks = rows // CHUNK
    dma = pltpu.SemaphoreType.DMA
    blocks = 2 * inner // COLS
    return pl.pallas_call(
        functools.partial(kernel, n, span),
        out_shape=jax.ShapeDtypeStruct((rows, inner), bf16),
        in_specs=[hbm] * 11,
        out_specs=vmem,
        scratch_shapes=[
            pltpu.SMEM(lengths.shape, jnp.int32),
            pltpu.VMEM((1, heads), f32),
            pltpu.VMEM((1, heads), f32),
            pltpu.VMEM(conv_weight.shape, f32),
            pltpu.VMEM((1024 * pl.cdiv(width, 1024),), f32),
            pltpu.VMEM((1, heads), f32),
            pltpu.VMEM((1024 * pl.cdiv(inner, 1024),), f32),
            pltpu.VMEM((rows, LANES), f32),
            pltpu.VMEM((rows + HALO, depth), bf16),
            pltpu.VMEM((depth, 2 * inner), bf16),
            pltpu.VMEM((depth, 2 * state), bf16),
            pltpu.VMEM((heads, depth), bf16),
            pltpu.VMEM((rows + 24 + 8 * ((chunks + 7) // 8), LANES), f32),
            pltpu.VMEM((rows + HALO, width), f32),
            pltpu.VMEM((3, rows, LANES), f32),
            pltpu.VMEM((rows, width), bf16),
            pltpu.VMEM((rows, inner), f32),
            pltpu.VMEM((rows, inner), f32),
            pltpu.VMEM((rows, inner), f32),
            pltpu.VMEM((chunks + 1, state, inner), f32),
            pltpu.VMEM((state, inner), bf16),
            pltpu.VMEM(small, f32),
            pltpu.VMEM((half, inner), bf16),
            pltpu.VMEM(small, f32),
            pltpu.VMEM((half, inner), bf16),
            pltpu.VMEM(small, f32),
            pltpu.VMEM((span, half, inner), bf16),
            pltpu.VMEM((span,) + small, f32),
            pltpu.VMEM((half, inner), bf16),
            pltpu.VMEM((state, inner), bf16),
            dma((8 + blocks + (width + inner) // LANES,)),
            dma((2,)),
            dma((4,)),
            dma((2 * span,)),
            dma((2 * span,)),
            dma((2,)),
        ],
        compiler_params=pltpu.CompilerParams(
            collective_id=0, has_side_effects=True, vmem_limit_bytes=60 * 1024 * 1024
        ),
        name="layer",
    )(
        tokens,
        lengths,
        gate_value_proj,
        state_proj,
        step_proj.T,
        step_bias[None],
        decay_log[None],
        conv_weight,
        conv_bias,
        skip_gain[None],
        norm_gain,
    )


def solution(mesh):
    return jax.shard_map(
        shards,
        mesh=mesh,
        in_specs=(P(("parts", "seq"), None), P("parts")) + (P(),) * 9,
        out_specs=P(("parts", "seq"), None),
        check_vma=False,
    )
```

```python
import functools

import jax
import jax.numpy as jnp
from jax import lax
from jax.experimental import pallas as pl
from jax.experimental.pallas import tpu as pltpu
from jax.sharding import PartitionSpec as P

CHUNK = 128
LANES = 128
HALO = 16
COLS = 256
MESH = pl.DeviceIdType.MESH
f32 = jnp.float32
bf16 = jnp.bfloat16


def split3(x):
    hi = x.astype(bf16)
    rest = x - hi.astype(f32)
    mid = rest.astype(bf16)
    return hi, mid, (rest - mid.astype(f32)).astype(bf16)


def expanded(x, spread):
    hi = x.astype(bf16)
    lo = (x - hi.astype(f32)).astype(bf16)
    return jnp.dot(jnp.concatenate([hi, lo], axis=1), spread, preferred_element_type=f32)


def half_silu(h):
    return h + h * jnp.tanh(h)


def kernel(
    n,
    span,
    tokens,
    lengths_hbm,
    gv_hbm,
    sp_hbm,
    stp_hbm,
    step_bias_hbm,
    decay_log_hbm,
    conv_weight_hbm,
    conv_bias_hbm,
    skip_gain_hbm,
    norm_gain_hbm,
    out,
    lengths,
    step_bias,
    decay_log,
    conv_weight,
    conv_bias,
    skip_gain,
    norm_gain,
    leave,
    tok,
    gv,
    sp,
    stp,
    narrow,
    mixed,
    keep,
    conv,
    gate,
    ysum,
    enter,
    state32,
    state16,
    dec_mine,
    pair16,
    pair_dec,
    got_a,
    got_a_dec,
    got_b,
    got_b_dec,
    enter16,
    full16,
    load_sem,
    halo_sem,
    a_sem,
    b_send,
    b_recv,
    c_sem,
):
    rows = tokens.shape[0]
    inner = gate.shape[1]
    width = conv.shape[1]
    state = (width - inner) // 2
    half = state // 2
    heads = stp.shape[0]
    head = inner // heads
    docs = lengths.shape[0]
    chunks = rows // CHUNK
    me = lax.axis_index("seq")
    core = lax.rem(me, 2)
    mate = me + 1 - 2 * core
    first = me * rows

    blocks = list(range(0, 2 * inner, COLS))
    order = [b for b in blocks if b >= inner]
    order += [b for b in blocks if b < inner < b + COLS]
    order += [b for b in blocks if b + COLS <= inner]
    loads = {}

    def load(name, src, dst):
        loads[name] = pltpu.make_async_copy(src, dst, load_sem.at[len(loads)])
        loads[name].start()

    load("lengths", lengths_hbm, lengths)
    load("stp", stp_hbm, stp)
    load("tok", tokens, tok.at[pl.ds(HALO, rows)])
    smalls = [
        (step_bias_hbm, step_bias),
        (decay_log_hbm, decay_log),
        (skip_gain_hbm, skip_gain),
        (conv_weight_hbm, conv_weight),
    ]
    for src, dst in ((conv_bias_hbm, conv_bias), (norm_gain_hbm, norm_gain)):
        for i in range(0, src.shape[0], LANES):
            smalls.append((src.at[pl.ds(i, LANES)], dst.at[pl.ds(i, LANES)]))
    for i, (src, dst) in enumerate(smalls):
        load(("small", i), src, dst)
    load("sp", sp_hbm, sp)
    for b in order:
        load(b, gv_hbm.at[:, pl.ds(b, COLS)], gv.at[:, pl.ds(b, COLS)])

    offsets = [-1, 1] + [s * 2 * k for k in range(1, span + 1) for s in (-1, 1)]
    barrier = pltpu.get_barrier_semaphore()
    for o in offsets:
        @pl.when((me + o >= 0) & (me + o < n))
        def _(o=o):
            pl.semaphore_signal(barrier, inc=1, device_id={"seq": me + o}, device_id_type=MESH)
    peers = jnp.int32(0)
    for o in offsets:
        peers = peers + jnp.where((me + o >= 0) & (me + o < n), 1, 0)
    pl.semaphore_wait(barrier, peers)

    halo = pltpu.make_async_remote_copy(
        src_ref=tokens.at[pl.ds(rows - HALO, HALO)],
        dst_ref=tok.at[pl.ds(0, HALO)],
        send_sem=halo_sem.at[0],
        recv_sem=halo_sem.at[1],
        device_id={"seq": lax.rem(me + 1, n)},
        device_id_type=MESH,
    )

    @pl.when(me + 1 < n)
    def _():
        halo.start()

    @pl.when(me == 0)
    def _():
        tok[0:HALO, :] = jnp.zeros((HALO, tok.shape[1]), tok.dtype)

    loads["lengths"].wait()
    starts = []
    total = jnp.int32(0)
    for j in range(docs):
        starts.append(total)
        total = total + lengths[j]
    pos = first + lax.broadcasted_iota(jnp.int32, (rows, LANES), 0)
    begin = jnp.zeros((rows, LANES), jnp.int32)
    for s in starts[1:]:
        begin = jnp.where(pos >= s, s, begin)

    def begin_of(p):
        b = jnp.int32(0)
        for s in starts[1:]:
            b = jnp.where(p >= s, s, b)
        return b

    for k in range(3):
        keep[k] = (pos - 3 + k >= begin).astype(f32)

    r = lax.broadcasted_iota(jnp.int32, (2 * LANES, inner), 0)
    c = lax.broadcasted_iota(jnp.int32, (2 * LANES, inner), 1)
    spread = (lax.rem(r, LANES) == c // head).astype(bf16)
    row_i = lax.broadcasted_iota(jnp.int32, (CHUNK, CHUNK), 0)
    col_i = lax.broadcasted_iota(jnp.int32, (CHUNK, CHUNK), 1)
    lower = (row_i >= col_i).astype(bf16)
    lower3 = jnp.concatenate([lower, lower, lower], axis=1)

    narrow[...] = jnp.zeros_like(narrow)
    for i in range(len(smalls)):
        loads["small", i].wait()
    loads["stp"].wait()
    loads["tok"].wait()
    own = tok.at[pl.ds(HALO, rows)]
    raw = lax.dot_general(
        own[...], stp[...], (((1,), (1,)), ((), ())), preferred_element_type=f32
    )
    narrow[0:rows, 0:heads] = raw
    narrow[rows : rows + 1, 0:heads] = step_bias[...]
    narrow[rows + 8 : rows + 9, 0:heads] = decay_log[...]
    narrow[rows + 16 : rows + 17, 0:heads] = skip_gain[...]
    @pl.when(me > 0)
    def _():
        halo.wait_recv()

    loads["sp"].wait()
    both = jnp.dot(tok[...], sp[...], preferred_element_type=f32)
    mixed[:, inner:width] = both.astype(bf16).astype(f32)

    live = lax.broadcasted_iota(jnp.int32, (CHUNK, LANES), 1) < heads
    rate = jnp.exp(narrow[rows + 8 : rows + 9, :])
    skip_row = expanded(narrow[rows + 16 : rows + 24, :], spread)[0:1]
    cums, cums_t, steps_t = [], [], []
    for ch in range(chunks):
        at = slice(ch * CHUNK, (ch + 1) * CHUNK)
        shifted = narrow[at, :] + narrow[rows : rows + 1, :]
        step = jnp.maximum(shifted, 0.0) + jnp.log1p(jnp.exp(-jnp.abs(shifted)))
        step = jnp.where(live, step, 0.0)
        cum = jnp.dot(
            lower3, jnp.concatenate(split3(-step * rate), axis=0), preferred_element_type=f32
        )
        cums.append(cum)
        cums_t.append(cum.T)
        steps_t.append(step.T)
        chunk_first = first + ch * CHUNK
        last_begin = begin_of(chunk_first + CHUNK - 1)
        here = first + ch * CHUNK + row_i
        leave[at, :] = (
            jnp.where(here >= last_begin, jnp.exp(cum[CHUNK - 1 : CHUNK] - cum), 0.0) * step
        )
        reach = jnp.where(begin[at] < chunk_first, jnp.exp(cum), 0.0)
        enter[at, 0:LANES] = reach
        narrow[rows + 24 + ch : rows + 25 + ch, :] = reach[CHUNK - 1 : CHUNK]
    wide_decs = expanded(narrow[rows + 24 : rows + 24 + 8 * ((chunks + 7) // 8), :], spread)
    decs = [wide_decs[ch : ch + 1] for ch in range(chunks)]

    bias_row = 0.5 * conv_bias[0:width].reshape(1, width)
    gain_row = norm_gain[0:inner].reshape(1, inner)

    piece = 64

    def convolve(lo_col, count):
        for col in range(lo_col, lo_col + count, LANES):
            cols = slice(col, col + LANES)
            w = 0.5 * conv_weight[:, cols]
            bias = bias_row[:, cols]
            for at in range(0, rows, piece):
                h = bias + w[3:4] * mixed[HALO + at : HALO + at + piece, cols]
                for k in range(3):
                    low = HALO - 3 + k + at
                    h = h + w[k : k + 1] * (
                        keep[k, at : at + piece, :] * mixed[low : low + piece, cols]
                    )
                conv[at : at + piece, cols] = half_silu(h).astype(bf16)

    def states(lo_col, count):
        cols = slice(lo_col, lo_col + count)
        total = None
        for ch in range(chunks):
            at = slice(ch * CHUNK, (ch + 1) * CHUNK)
            weighted = conv[at, cols].astype(f32) * expanded(leave[at, :], spread[:, cols])
            own_state = lax.dot_general(
                conv[at, inner : inner + state],
                weighted.astype(bf16),
                (((0,), (0,)), ((), ())),
                preferred_element_type=f32,
            )
            state32[ch, :, cols] = own_state
            total = own_state if ch == 0 else decs[ch][:, cols] * total + own_state
        state32[chunks, :, cols] = total
        state16[:, cols] = total.astype(bf16)

    pending = [(inner, width - inner)]
    for b in order:
        if b + COLS <= inner:
            continue
        loads[b].wait()
        got = jnp.dot(tok[...], gv[:, b : b + COLS], preferred_element_type=f32)
        gates = max(0, inner - b)
        if gates:
            gate[:, b:inner] = 0.5 * got[HALO:, :gates].astype(bf16).astype(f32)
        mixed[:, b + gates - inner : b + COLS - inner] = (
            got[:, gates:].astype(bf16).astype(f32)
        )
        for p in pending:
            convolve(*p)
            if p[0] < inner:
                states(*p)
        pending = [(b + gates - inner, COLS - gates)]
    for p in pending:
        convolve(*p)
        states(*p)
    device_dec = decs[0]
    for ch in range(1, chunks):
        device_dec = decs[ch] * device_dec

    def put_row(ref, row):
        for j in range(inner // LANES):
            ref[j : j + 1, :] = row[:, j * LANES : (j + 1) * LANES]

    def get_row(block):
        return jnp.concatenate([block[j : j + 1] for j in range(inner // LANES)], axis=1)

    put_row(dec_mine, device_dec)
    mine_at = pl.multiple_of(core * half, half)
    mate_at = pl.multiple_of((1 - core) * half, half)

    def remote(src, dst, send, recv, target):
        return pltpu.make_async_remote_copy(
            src_ref=src,
            dst_ref=dst,
            send_sem=send,
            recv_sem=recv,
            device_id={"seq": target},
            device_id_type=MESH,
        )

    a_copy = remote(state16.at[pl.ds(mate_at, half)], got_a, a_sem.at[0], a_sem.at[1], mate)
    a_dec = remote(dec_mine, got_a_dec, a_sem.at[2], a_sem.at[3], mate)
    a_copy.start()
    a_dec.start()

    def inside(ch):
        at = slice(ch * CHUNK, (ch + 1) * CHUNK)
        in_map = conv[at, inner : inner + state]
        out_map = conv[at, inner + state : width]
        scores = lax.dot_general(
            out_map, in_map, (((1,), (1,)), ((), ())), preferred_element_type=f32
        )
        allowed = (row_i >= col_i) & (first + ch * CHUNK + col_i >= begin[at])
        lane = lax.broadcasted_iota(jnp.int32, (CHUNK, LANES), 1)
        per = LANES // head
        for tile in range(inner // LANES):
            x = conv[at, tile * LANES : (tile + 1) * LANES]
            mixes, values = [], []
            for i in range(per):
                h = tile * per + i
                diff = jnp.minimum(cums[ch][:, h : h + 1] - cums_t[ch][h : h + 1, :], 0.0)
                weight = jnp.where(allowed, jnp.exp(diff), 0.0)
                mixes.append((weight * scores * steps_t[ch][h : h + 1, :]).astype(bf16))
                values.append(jnp.where(lane // head == i, x, jnp.zeros_like(x)))
            y = jnp.dot(
                jnp.concatenate(mixes, axis=1),
                jnp.concatenate(values, axis=0),
                preferred_element_type=f32,
            )
            cols = slice(tile * LANES, (tile + 1) * LANES)
            ysum[at, cols] = y + skip_row[:, cols] * x.astype(f32)

    def widen(ch):
        at = slice(ch * CHUNK, (ch + 1) * CHUNK)
        enter[at, :] = expanded(enter[at, 0:LANES], spread)

    inside(0)

    a_copy.wait()
    a_dec.wait()
    theirs = got_a[...].astype(f32)
    theirs_dec = get_row(got_a_dec[...])
    mine = state32[chunks, pl.ds(mine_at, half), :]
    even = core == 0
    early = jnp.where(even, mine, theirs)
    early_dec = jnp.where(even, device_dec, theirs_dec)
    late = jnp.where(even, theirs, mine)
    late_dec = jnp.where(even, theirs_dec, device_dec)
    pair16[...] = (late + late_dec * early).astype(bf16)
    put_row(pair_dec, late_dec * early_dec)

    b_copies = []
    for k in range(1, span + 1):
        target = lax.rem(me + 2 * k, n)
        b_copies.append(
            (
                remote(pair16, got_b.at[k - 1], b_send.at[2 * k - 2], b_recv.at[2 * k - 2], target),
                remote(
                    pair_dec, got_b_dec.at[k - 1], b_send.at[2 * k - 1], b_recv.at[2 * k - 1], target
                ),
            )
        )
    for k in range(1, span + 1):
        @pl.when(me + 2 * k < n)
        def _(k=k):
            for cp in b_copies[k - 1]:
                cp.start()

        @pl.when(me - 2 * k < 0)
        def _(k=k):
            got_b[k - 1] = jnp.zeros(got_b.shape[1:], bf16)
            got_b_dec[k - 1] = jnp.zeros(got_b_dec.shape[1:], f32)

    for b in order:
        if b + COLS > inner:
            continue
        loads[b].wait()
        got = jnp.dot(own[...], gv[:, b : b + COLS], preferred_element_type=f32)
        gate[:, b : b + COLS] = 0.5 * got.astype(bf16).astype(f32)
    for ch in range(1, chunks):
        inside(ch)
    for ch in range(chunks):
        at = slice(ch * CHUNK, (ch + 1) * CHUNK)
        widen(ch)
        gate[at, :] = half_silu(gate[at, :])

    for k in range(1, span + 1):
        @pl.when(me - 2 * k >= 0)
        def _(k=k):
            for cp in b_copies[k - 1]:
                cp.wait_recv()
    chip = jnp.zeros((half, inner), f32)
    for k in range(span, 0, -1):
        chip = got_b[k - 1].astype(f32) + get_row(got_b_dec[k - 1]) * chip
    second = early + early_dec * chip
    full16[pl.ds(mine_at, half), :] = jnp.where(even, chip, second).astype(bf16)
    enter16[...] = jnp.where(even, second, chip).astype(bf16)
    c_copy = remote(enter16, full16.at[pl.ds(mine_at, half)], c_sem.at[0], c_sem.at[1], mate)
    c_copy.start()
    c_copy.wait()

    carried = full16[...].astype(f32)
    for ch in range(chunks):
        at = slice(ch * CHUNK, (ch + 1) * CHUNK)
        off = jnp.dot(
            conv[at, inner + state : width], carried.astype(bf16), preferred_element_type=f32
        )
        gated = (ysum[at, :] + enter[at, :] * off) * gate[at, :]
        square = jnp.sum(gated * gated, axis=1, keepdims=True) * (1.0 / inner)
        out[at, :] = (gated * lax.rsqrt(square + 1e-05) * gain_row).astype(bf16)
        if ch + 1 < chunks:
            carried = decs[ch] * carried + state32[ch]

    @pl.when(me + 1 < n)
    def _():
        halo.wait_send()

    for k in range(1, span + 1):
        @pl.when(me + 2 * k < n)
        def _(k=k):
            for cp in b_copies[k - 1]:
                cp.wait_send()


def shards(
    tokens,
    lengths,
    gate_value_proj,
    state_proj,
    step_proj,
    step_bias,
    decay_log,
    conv_weight,
    conv_bias,
    skip_gain,
    norm_gain,
):
    rows, depth = tokens.shape
    inner = gate_value_proj.shape[1] // 2
    state = state_proj.shape[1] // 2
    heads = step_proj.shape[1]
    width = inner + 2 * state
    n = lax.axis_size("seq")
    span = max(1, n // 8)
    hbm = pl.BlockSpec(memory_space=pltpu.HBM)
    vmem = pl.BlockSpec(memory_space=pltpu.VMEM)
    half = state // 2
    small = (8, LANES)
    chunks = rows // CHUNK
    dma = pltpu.SemaphoreType.DMA
    blocks = 2 * inner // COLS
    return pl.pallas_call(
        functools.partial(kernel, n, span),
        out_shape=pltpu.VMEM((rows, inner), bf16),
        in_specs=[hbm] * 11,
        out_specs=vmem,
        scratch_shapes=[
            pltpu.SMEM(lengths.shape, jnp.int32),
            pltpu.VMEM((1, heads), f32),
            pltpu.VMEM((1, heads), f32),
            pltpu.VMEM(conv_weight.shape, f32),
            pltpu.VMEM((1024 * pl.cdiv(width, 1024),), f32),
            pltpu.VMEM((1, heads), f32),
            pltpu.VMEM((1024 * pl.cdiv(inner, 1024),), f32),
            pltpu.VMEM((rows, LANES), f32),
            pltpu.VMEM((rows + HALO, depth), bf16),
            pltpu.VMEM((depth, 2 * inner), bf16),
            pltpu.VMEM((depth, 2 * state), bf16),
            pltpu.VMEM((heads, depth), bf16),
            pltpu.VMEM((rows + 24 + 8 * ((chunks + 7) // 8), LANES), f32),
            pltpu.VMEM((rows + HALO, width), f32),
            pltpu.VMEM((3, rows, LANES), f32),
            pltpu.VMEM((rows, width), bf16),
            pltpu.VMEM((rows, inner), f32),
            pltpu.VMEM((rows, inner), f32),
            pltpu.VMEM((rows, inner), f32),
            pltpu.VMEM((chunks + 1, state, inner), f32),
            pltpu.VMEM((state, inner), bf16),
            pltpu.VMEM(small, f32),
            pltpu.VMEM((half, inner), bf16),
            pltpu.VMEM(small, f32),
            pltpu.VMEM((half, inner), bf16),
            pltpu.VMEM(small, f32),
            pltpu.VMEM((span, half, inner), bf16),
            pltpu.VMEM((span,) + small, f32),
            pltpu.VMEM((half, inner), bf16),
            pltpu.VMEM((state, inner), bf16),
            dma((8 + blocks + (width + inner) // LANES,)),
            dma((2,)),
            dma((4,)),
            dma((2 * span,)),
            dma((2 * span,)),
            dma((2,)),
        ],
        compiler_params=pltpu.CompilerParams(
            collective_id=0, has_side_effects=True, vmem_limit_bytes=66_000_000
        ),
        name="layer",
    )(
        tokens,
        lengths,
        gate_value_proj,
        state_proj,
        step_proj.T,
        step_bias[None],
        decay_log[None],
        conv_weight,
        conv_bias,
        skip_gain[None],
        norm_gain,
    )


def solution(mesh):
    return jax.shard_map(
        shards,
        mesh=mesh,
        in_specs=(P(("parts", "seq"), None), P("parts")) + (P(),) * 9,
        out_specs=P(("parts", "seq"), None),
        check_vma=False,
    )
```
